32 devices in a mesh: context: 8 (over z, y), tensor: 4 (over x, core).
Axes of the slice: x: 2, y: 2, z: 4, core: 2. Of those that a mesh axis runs over, the one named last changes fastest.
Arguments:
- hidden: bfloat16 [256, 4096], P('context', 'tensor'), may hold values from -270 to 270
- weight: bfloat16 [4096, 128256], P(None, ('context', 'tensor')), may hold values from -0.25 to 0.25
- targets: int32 [256], P('context'), may hold values from 0 to 128255
- mask: int32 [256], P('context'), may hold values 0 or 1
- loss_scale: float32 [], replicated, may hold values from 2048 to 32768
Outputs:
- loss: float32 [], replicated
- grad_hidden: bfloat16 [256, 4096], P('context', 'tensor')
- grad_weight: bfloat16 [4096, 128256], P(None, ('context', 'tensor'))
The draws below stay inside these ranges and needn't reach their ends.
All inputs are finite; a program needn't handle non-finite values. No bound on the sum of `mask` on one device may be relied on, other than what follows from the above.
Results may differ from the reference program's by a relative error of at most 0.0052.
Values may be sent and summed in bfloat16 or wider, within the bound.
No kernel may reach another device: no remote copies, remote signals or barrier semaphores. Data moves between devices by JAX's collectives and lax.ppermute only.
A program may use at most 192 MiB of HBM per device.

```python
import math
import jax
import jax.numpy as jnp
import numpy as np
from jax import lax

D = 4096
V = 128256
TOKENS = 256


def draw_hidden(key, part):
    keys = jax.random.split(jax.random.fold_in(key, 11), 1)
    base = jnp.clip(jax.random.normal(keys[0], (TOKENS, D), jnp.float32), -6.0, 6.0)
    values = base
    return values.astype(jnp.bfloat16)


def touch_ends(values, stream_key, low, top_value):
    longest = values.shape.index(max(values.shape))
    spots = []
    for shift in (0, 1):
        where = [jax.random.randint(jax.random.fold_in(stream_key, axis), (), 0, length) for axis, length in enumerate(values.shape)]
        where[longest] = (where[longest] + shift) % values.shape[longest]
        spots.append(tuple(where))
    return values.at[spots[0]].set(low).at[spots[1]].set(top_value)


def block_scale(rng, dims, pieces, smallest, top_value):
    gain = 1.0
    for axis_at, parts in pieces:
        heights = jax.random.uniform(jax.random.fold_in(jax.random.fold_in(rng, 6), axis_at), (parts,), jnp.float32, smallest / len(pieces), top_value / len(pieces))
        gain = gain * jnp.repeat(jnp.exp(heights), dims[axis_at] // parts).reshape((-1,) + (1,) * (len(dims) - 1 - axis_at))
    return gain


def skewed_wide(own_key, extent, amount, skew):
    weights = [min(1 << octave, amount + 1 - (1 << octave)) * (1 << 20) // math.isqrt((1 << octave) ** skew) + 1 for octave in range((amount + 1).bit_length()) if 1 << octave <= amount]
    spread = 1 + sum(weights) // (1 << 30)
    grid = np.cumsum(np.array([max(1, weight // spread) for weight in weights]))
    ticket = jax.random.randint(jax.random.fold_in(own_key, 1), extent, 0, int(grid[len(weights) - 1]))
    start = jnp.left_shift(1, jnp.searchsorted(jnp.asarray(grid, jnp.int32), ticket, side="right").astype(jnp.int32))
    grade = start - 1 + jax.random.randint(jax.random.fold_in(own_key, 4), extent, 0, 1 << 30) % jnp.minimum(start, amount + 1 - start)
    return jax.random.permutation(jax.random.fold_in(own_key, 2), amount)[grade].astype(jnp.int32)


def noise(stream_key, shape, deviation, limit, cuts=(), kind=jnp.bfloat16):
    drawn = deviation * jax.random.normal(stream_key, shape, jnp.float32)
    if cuts:
        drawn = drawn * block_scale(stream_key, shape, cuts, -0.22, 0.18)
    return jnp.clip(drawn, -limit, limit).astype(kind)


def setup_inputs(seed: int = 0) -> dict:
    splits = jax.random.split(jax.random.key(seed), 6)
    return {
        "hidden": draw_hidden(jax.random.fold_in(splits[5], 71), 0),
        "weight": noise(splits[1], (D, V), (D // 9) ** -0.5, 0.25, ((1, 32),)),
        "targets": touch_ends(skewed_wide(splits[2], (TOKENS,), V, 2), jax.random.fold_in(splits[2], 3), 0, V - 1).astype(jnp.int32),
        "mask": touch_ends((jax.random.randint(splits[3], (TOKENS,), 0, 4) < 3).astype(jnp.int32), jax.random.fold_in(splits[3], 1), 0, 1),
        "loss_scale": jnp.clip(jnp.exp(jax.random.uniform(splits[4], (), jnp.float32, math.log(2048.0), math.log(32768.0))), 2048.0, 32768.0),
    }


clip_limit = 1.0

def reference(hidden, weight, targets, mask, loss_scale):
    logits = jnp.dot(hidden, weight, preferred_element_type=jnp.float32)
    row_max = lax.optimization_barrier(jnp.max(logits, axis=1))
    shifted = jnp.exp(logits - row_max[:, None])
    sum_exp = lax.optimization_barrier(jnp.sum(shifted, axis=1))
    target_logit = jnp.take_along_axis(logits, targets.astype(jnp.int32)[:, None], axis=1)[:, 0]
    token_loss = jnp.log(sum_exp) + row_max - target_logit
    maskf = mask.astype(jnp.float32)
    denom = jnp.maximum(jnp.sum(maskf), jnp.float32(1.0))
    loss = jnp.sum(maskf * token_loss) / denom
    columns = lax.broadcasted_iota(jnp.int32, (1, logits.shape[1]), 1)
    onehot = (columns == targets.astype(jnp.int32)[:, None]).astype(jnp.float32)
    factor = loss_scale * maskf / denom
    grad_logits = (factor[:, None] * (shifted / sum_exp[:, None] - onehot)).astype(jnp.bfloat16)
    grad_hidden = lax.dot_general(grad_logits, weight, (((1,), (1,)), ((), ())), preferred_element_type=jnp.float32).astype(jnp.bfloat16)
    raw_grad = lax.dot_general(hidden, grad_logits, (((0,), (0,)), ((), ())), preferred_element_type=jnp.float32)
    grad_norm = jnp.sqrt(jnp.sum(raw_grad * raw_grad)) / loss_scale
    grad_weight = (raw_grad * (clip_limit / jnp.maximum(grad_norm, clip_limit))).astype(jnp.bfloat16)
    return (loss, grad_hidden, grad_weight)
```

```python
import functools

import jax
import jax.numpy as jnp
from jax import lax
from jax.experimental import pallas as pl
from jax.experimental.pallas import tpu as pltpu
from jax.sharding import PartitionSpec as P

clip_limit = 1.0
both = ("context", "tensor")
lowest = -1e30
f32 = jnp.float32
bf16 = jnp.bfloat16


def cost(flops, moved):
    return pl.CostEstimate(flops=int(flops), bytes_accessed=int(moved), transcendentals=0)


def divisor(size, most):
    best = size
    while best > most and best % 2 == 0:
        best //= 2
    return best


def hop(value, ctx, ten, dz, dy, dx, dc):
    pairs = []
    for source in range(ctx * ten):
        place, part = divmod(source, ten)
        other = ((place // 2 ^ dz) * 2 + (place % 2 ^ dy)) * ten
        pairs.append((source, other + (part // 2 ^ dx) * 2 + (part % 2 ^ dc)))
    return lax.ppermute(value, both, pairs)


def gathered(hidden, ctx, ten):
    levels = ctx // 2
    half = levels // 2
    go = functools.partial(hop, ctx=ctx, ten=ten)
    mine = jnp.stack(
        [hidden] + [go(hidden, dz=d, dy=0, dx=0, dc=0) for d in range(1, levels)]
    )
    across = go(mine, dz=0, dy=0, dx=1, dc=0)
    beside = go(mine, dz=0, dy=1, dx=0, dc=0)
    low = go(beside[:half], dz=0, dy=0, dx=1, dc=0)
    high = go(across[half:], dz=0, dy=1, dx=0, dc=0)
    found = [
        (mine, 0, 0, 0),
        (across, 0, 1, 0),
        (beside, 0, 0, 1),
        (low, 0, 1, 1),
        (high, half, 1, 1),
    ]
    pieces, places = [], []
    for flip in (0, 1):
        for block, first, dx, dy in found:
            pieces.append(go(block, dz=0, dy=0, dx=0, dc=1) if flip else block)
            places.append((tuple(range(first, first + block.shape[0])), dx, dy, flip))
    return pieces, tuple(places)


def logits_kernel(places, vocab, steps, at_ref, own_ref, *refs):
    pieces = refs[: len(places)]
    weight_ref, logits_ref, note_ref, hidden_ref, gram_ref, top_ref, sum_ref, sems = refs[
        len(places) :
    ]
    step = pl.program_id(0)
    z, y, x, c = (at_ref[k] for k in range(4))

    @pl.when(step == 0)
    def _():
        copies = []
        for piece, (levels, dx, dy, dc) in zip(pieces, places):
            _, rows, width = piece.shape
            for k, dz in enumerate(levels):
                row = pl.multiple_of(((z ^ dz) * 2 + (y ^ dy)) * rows, rows)
                column = pl.multiple_of(((x ^ dx) * 2 + (c ^ dc)) * width, width)
                copies.append(
                    pltpu.make_async_copy(
                        piece.at[k],
                        hidden_ref.at[pl.ds(row, rows), pl.ds(column, width)],
                        sems.at[len(copies)],
                    )
                )
        for copy in copies:
            copy.start()
        top_ref[...] = jnp.full_like(top_ref, lowest)
        sum_ref[...] = jnp.zeros_like(sum_ref)
        for copy in copies:
            copy.wait()
        gram_ref[...] = lax.dot_general(
            hidden_ref[...],
            hidden_ref[...],
            (((1,), (1,)), ((), ())),
            preferred_element_type=f32,
        )

    logits = lax.dot_general(
        weight_ref[...],
        hidden_ref[...],
        (((1,), (1,)), ((), ())),
        preferred_element_type=f32,
    )
    block = logits.shape[0]
    entries = step * block + lax.broadcasted_iota(jnp.int32, logits.shape, 0)
    logits = jnp.where(entries < vocab, logits, lowest)
    logits_ref[...] = logits
    old = top_ref[:1]
    top = jnp.maximum(old, jnp.max(logits, axis=0, keepdims=True))
    shifted = jnp.sum(jnp.exp(logits - top), axis=0, keepdims=True)
    sum_ref[:1] = sum_ref[:1] * jnp.exp(old - top) + shifted
    top_ref[:1] = top

    @pl.when(step == steps - 1)
    def _():
        rows = jnp.concatenate([top_ref[:1], sum_ref[:1], own_ref[2:]], axis=0)
        for device in range(note_ref.shape[0]):
            note_ref[device] = rows


def gradient_kernel(
    vocab, block, at_ref, notes_ref, scale_ref, logits_ref, gram_ref, weight_ref,
    part_ref, grad_ref, turned_ref, sums_ref,
):
    @pl.when(pl.program_id(0) == 0)
    def _():
        offset = at_ref[4]
        notes = notes_ref[...]
        tops = notes[:, 0, :]
        top = jnp.max(tops, axis=0, keepdims=True)
        total = jnp.sum(notes[:, 1, :] * jnp.exp(tops - top), axis=0, keepdims=True)
        target = jnp.sum(notes[:, 2, :], axis=0, keepdims=True)
        mask = jnp.sum(notes[:, 3, :], axis=0, keepdims=True)
        denom = jnp.maximum(jnp.sum(mask, axis=1, keepdims=True), 1.0)
        factor = scale_ref[0, 0] * mask / denom
        rate = factor / total
        known = jnp.sum(mask * (jnp.log(total) + top), axis=1, keepdims=True)
        spot = target.astype(jnp.int32) - offset
        spot = jnp.where(spot < vocab, spot, -1)
        gram = jnp.zeros(gram_ref.shape, f32)
        hit = jnp.zeros(spot.shape, f32)
        for start in range(0, logits_ref.shape[0], block):
            logits = logits_ref[start : start + block]
            entries = start + lax.broadcasted_iota(jnp.int32, logits.shape, 0)
            chosen = entries == spot
            hit += jnp.sum(jnp.where(chosen, logits, 0.0), axis=0, keepdims=True)
            grad = rate * jnp.exp(logits - top) - jnp.where(chosen, factor, 0.0)
            grad = grad.astype(bf16)
            grad_ref[start : start + block] = grad
            turned = jnp.transpose(grad)
            turned_ref[:, start : start + block] = turned
            gram += jnp.dot(turned, grad, preferred_element_type=f32)
        squares = jnp.sum(
            jnp.sum(gram * gram_ref[...], axis=1, keepdims=True), axis=0, keepdims=True
        )
        hits = jnp.sum(mask * hit, axis=1, keepdims=True)
        lanes = lax.broadcasted_iota(jnp.int32, sums_ref.shape, 1)
        sums_ref[...] = jnp.where(
            lanes == 0,
            squares,
            jnp.where(lanes == 1, hits, jnp.where(lanes == 2, known, denom)),
        )

    part_ref[0] = jnp.dot(
        turned_ref[:, :vocab], weight_ref[...], preferred_element_type=f32
    ).astype(part_ref.dtype)


def product_kernel(vocab, at_ref, turned_ref, weight_ref, part_ref):
    part_ref[0] = jnp.dot(
        turned_ref[:, :vocab], weight_ref[...], preferred_element_type=f32
    ).astype(part_ref.dtype)


def outer_kernel(width, rate_ref, hidden_ref, grad_ref, out_ref):
    rate = rate_ref[0, 0]
    for start in range(0, out_ref.shape[1], width):
        raw = jnp.dot(
            grad_ref[...], hidden_ref[:, start : start + width], preferred_element_type=f32
        )
        out_ref[:, start : start + width] = (raw * rate).astype(bf16)


def encoded(values):
    first = lax.reduce_precision(values, 8, 7)
    second = lax.reduce_precision(values - first, 8, 7)
    third = lax.reduce_precision(values - first - second, 8, 7)
    return jnp.concatenate([first, second, third])


def decoded(row, count):
    terms = row[: 3 * count].astype(f32)
    return terms[:count] + terms[count : 2 * count] + terms[2 * count :]


def packed(block, values, width):
    flat = block.astype(bf16).reshape(-1, width)
    row = jnp.pad(encoded(values), (0, width - 3 * values.shape[0])).astype(bf16)
    return jnp.concatenate([flat, jnp.broadcast_to(row[None], (8, width))])


def shards(ctx, ten, hidden, weight, targets, mask, loss_scale):
    rows, width = hidden.shape
    model, vocab = weight.shape
    table = weight.T
    tokens = rows * ctx
    devices = ctx * ten
    levels = ctx // 2
    half = levels // 2
    place, part = lax.axis_index("context"), lax.axis_index("tensor")
    z, y, x, c = place // 2, place % 2, part // 2, part % 2
    offset = (place * ten + part) * vocab
    at = jnp.stack([z, y, x, c, offset]).astype(jnp.int32)
    go = functools.partial(hop, ctx=ctx, ten=ten)

    own = jnp.stack([targets, mask]).astype(f32) * (part == 0).astype(f32)
    own = lax.dynamic_update_slice(
        jnp.zeros((8, tokens), f32), own, (jnp.int32(2), (place * rows).astype(jnp.int32))
    )
    pieces, places = gathered(hidden, ctx, ten)
    block = 512
    steps = pl.cdiv(vocab, block)
    padded = steps * block
    full = lambda *shape: pl.BlockSpec(shape, lambda i, s: (0,) * len(shape))
    anywhere = pl.BlockSpec(memory_space=pl.ANY)
    smem = pl.BlockSpec(memory_space=pltpu.SMEM)
    count = sum(len(p[0]) for p in places)
    logits, note, whole, gram = pl.pallas_call(
        functools.partial(logits_kernel, places, vocab, steps),
        grid_spec=pltpu.PrefetchScalarGridSpec(
            num_scalar_prefetch=1,
            grid=(steps,),
            in_specs=[full(8, tokens)]
            + [anywhere] * len(pieces)
            + [pl.BlockSpec((block, model), lambda i, s: (i, 0))],
            out_specs=[
                pl.BlockSpec((block, tokens), lambda i, s: (i, 0)),
                full(devices, 8, tokens),
                full(tokens, model),
                full(tokens, tokens),
            ],
            scratch_shapes=[
                pltpu.VMEM((8, tokens), f32),
                pltpu.VMEM((8, tokens), f32),
                pltpu.SemaphoreType.DMA((count,)),
            ],
        ),
        out_shape=[
            jax.ShapeDtypeStruct((padded, tokens), f32),
            jax.ShapeDtypeStruct((devices, 8, tokens), f32),
            jax.ShapeDtypeStruct((tokens, model), bf16),
            jax.ShapeDtypeStruct((tokens, tokens), f32),
        ],
        cost_estimate=cost(2 * tokens * model * vocab, 2 * model * vocab),
        name="logits",
    )(at, own, *pieces, table)

    notes = lax.all_to_all(note, both, 0, 0)

    tall = divisor(width, 512)
    inner = width // tall
    scale = loss_scale.reshape(1, 1)

    def block_rows(flip):
        def index(i, s):
            dx = i // inner
            group = (s[2] ^ dx) * 2 + (s[3] ^ flip)
            return (0, group * inner + i % inner)

        return pl.BlockSpec((vocab, tall), index)

    parts = pl.BlockSpec((1, tokens, tall), lambda i, s: (i // inner, 0, i % inner))
    sent, grad, turned, sums = pl.pallas_call(
        functools.partial(gradient_kernel, vocab, block),
        grid_spec=pltpu.PrefetchScalarGridSpec(
            num_scalar_prefetch=1,
            grid=(2 * inner,),
            in_specs=[
                full(devices, 8, tokens),
                smem,
                full(padded, tokens),
                full(tokens, tokens),
                block_rows(1),
            ],
            out_specs=[parts, full(padded, tokens), full(tokens, padded), full(8, 128)],
        ),
        out_shape=[
            jax.ShapeDtypeStruct((2, tokens, width), bf16),
            jax.ShapeDtypeStruct((padded, tokens), bf16),
            jax.ShapeDtypeStruct((tokens, padded), bf16),
            jax.ShapeDtypeStruct((8, 128), f32),
        ],
        cost_estimate=cost(tokens * model * vocab, model * vocab),
        name="gradient",
    )(at, notes, scale, logits, gram, table)
    came = go(sent, dz=0, dy=0, dx=0, dc=1)
    twin = go(sums, dz=0, dy=0, dx=0, dc=1)
    kept = pl.pallas_call(
        functools.partial(product_kernel, vocab),
        grid_spec=pltpu.PrefetchScalarGridSpec(
            num_scalar_prefetch=1,
            grid=(2 * inner,),
            in_specs=[full(tokens, padded), block_rows(0)],
            out_specs=parts,
        ),
        out_shape=jax.ShapeDtypeStruct((2, tokens, width), f32),
        cost_estimate=cost(tokens * model * vocab, model * vocab),
        name="product",
    )(at, turned, table)

    pair = sums[0, :2] + twin[0, :2]
    total = (kept + came.astype(f32)).reshape(2, levels, 2, rows, width)
    near = lambda dx, dy: lax.dynamic_index_in_dim(total[dx], y ^ dy, axis=1, keepdims=False)
    far = near(1, 1)
    shape = (-1, rows, width)
    open_up = lambda message: (
        message[:-8].reshape(shape).astype(f32),
        decoded(message[-8], 2),
    )
    from_x, pair_x = open_up(go(packed(far[:half], pair, width), dz=0, dy=0, dx=1, dc=0))
    from_y, pair_y = open_up(go(packed(far[half:], pair, width), dz=0, dy=1, dx=0, dc=0))
    for_x, for_y = near(1, 0), near(0, 1)
    for_x = jnp.concatenate([for_x[:half], for_x[half:] + from_y])
    for_y = jnp.concatenate([for_y[:half] + from_x, for_y[half:]])
    got_x, cross = open_up(go(packed(for_x, pair + pair_y, width), dz=0, dy=0, dx=1, dc=0))
    got_y = go(for_y.astype(bf16), dz=0, dy=1, dx=0, dc=0).astype(f32)
    layer = near(0, 0) + got_x + got_y
    quad = pair + pair_y + cross
    pick = lambda d: lax.dynamic_index_in_dim(layer, z ^ d, axis=0, keepdims=False)
    result, both_sums = pick(0), quad
    for d in range(1, levels):
        message, value = open_up(go(packed(pick(d), quad, width), dz=d, dy=0, dx=0, dc=0))
        result += message[0]
        both_sums += value
    grad_hidden = result.astype(bf16)

    squares, hits = both_sums[0], both_sums[1]
    loss = (sums[0, 2] - hits) / sums[0, 3]
    grad_norm = jnp.sqrt(jnp.maximum(squares, 0.0)) / loss_scale
    rate = (clip_limit / jnp.maximum(grad_norm, clip_limit)).reshape(1, 1)
    grad_weight = pl.pallas_call(
        functools.partial(outer_kernel, block),
        grid=(steps,),
        in_specs=[
            smem,
            pl.BlockSpec((tokens, model), lambda i: (0, 0)),
            pl.BlockSpec((block, tokens), lambda i: (i, 0)),
        ],
        out_specs=pl.BlockSpec((block, model), lambda i: (i, 0)),
        out_shape=jax.ShapeDtypeStruct((vocab, model), bf16),
        cost_estimate=cost(2 * tokens * model * vocab, 2 * model * vocab),
        name="outer",
    )(rate, whole, grad).T
    return (loss, grad_hidden, grad_weight)


def solution(mesh):
    placed = (
        P("context", "tensor"),
        P(None, both),
        P("context"),
        P("context"),
        P(),
    )
    return jax.shard_map(
        functools.partial(shards, mesh.shape["context"], mesh.shape["tensor"]),
        mesh=mesh,
        in_specs=placed,
        out_specs=(P(), P("context", "tensor"), P(None, both)),
        check_vma=False,
    )
```
